256 devices in a mesh: groups: 4 (over x, y), feat: 64 (over z, core).
Axes of the slice: x: 2, y: 2, z: 32, core: 2. Of those that a mesh axis runs over, the one named last changes fastest.
The devices are a block of a 4x8x32 slice.
Arguments:
- cells: bfloat16 [768, 512, 192], P('groups', 'feat'), parts along dimension 0, may hold values from -6 to 6
- missing: int32 [768, 512], P('groups', 'feat'), parts along dimension 0, may hold values 0 or 1
- feat_ids: int32 [2048], P(('groups', 'feat')), parts along dimension 0, may hold values from 0 to 63
- feat_table: float32 [64, 192], replicated, may hold values from -5 to 5
- nan_embed: float32 [192], replicated, may hold values from -5 to 5
- gain_one: float32 [192], replicated, may hold values from 0.1 to 1.9
- w_qkv: bfloat16 [192, 576], replicated, may hold values from -3 to 3
- w_out: bfloat16 [192, 192], replicated, may hold values from -0.4375 to 0.4375
- gain_two: float32 [192], replicated, may hold values from 0.1 to 1.9
- w_up: bfloat16 [192, 768], replicated, may hold values from -0.4375 to 0.4375
- w_down: bfloat16 [768, 192], replicated, may hold values from -0.21875 to 0.21875
Outputs:
- result: float32 [768, 512, 192], P('groups', 'feat'), parts along dimension 0
The draws below stay inside these ranges and needn't reach their ends.
There are 4 independent parts, one for each index of `groups`. The reference program is written for one: setup_inputs(seed, part) draws one part's arguments, and reference() takes and returns one part's arrays. A program takes and returns all parts, laid end to end along the dimension named above; an argument that names none is the same for every part. Nothing has to cross between parts.
All inputs are finite; a program needn't handle non-finite values. No bound on the sum of `missing` on one device may be relied on, other than what follows from the above.
Results may differ from the reference program's by a relative error of at most 0.007.
The reference program's roundings to bfloat16 on the way (of `tokens`, `normed`, `qkv`, `probs`, `context`, `normed_two` and `act`) count: a program that leaves them out, or rounds other values in their place, can miss the bound.
Values may be sent and summed in bfloat16 or wider, within the bound.
A program may use at most 64 MiB of HBM per device.

```python
import jax
import jax.numpy as jnp
from jax import lax

E = 192
HEADS = 6
MLP = 768
F = 512
NCAT = 64
R = 192


def draw_w_qkv(key, part):
    weights = jax.random.normal(key, (E, 3 * E), jnp.float32) * E ** (-0.5)
    return jnp.clip(weights, -3.0, 3.0).astype(jnp.bfloat16)


def touch_ends(values, key, smallest, top_value):
    longest = values.shape.index(max(values.shape))
    spots = []
    for shift in (0, 1):
        where = [jax.random.randint(jax.random.fold_in(key, axis), (), 0, length) for axis, length in enumerate(values.shape)]
        where[longest] = (where[longest] + shift) % values.shape[longest]
        spots.append(tuple(where))
    return values.at[spots[0]].set(smallest).at[spots[1]].set(top_value)


def block_scale(rng, extent, shards, smallest, high):
    def one(dim, parts):
        steps = jax.random.uniform(jax.random.fold_in(jax.random.fold_in(rng, 6), dim), (parts,), jnp.float32, smallest / len(shards), high / len(shards))
        return jnp.repeat(jnp.exp(steps), extent[dim] // parts).reshape((-1,) + (1,) * (len(extent) - dim - 1))

    loudness = one(*shards[0])
    for cut in shards[1:]:
        loudness = loudness * one(*cut)
    return loudness


def centred(stream_key, extent, spread, reach, pieces=(), held_as=jnp.bfloat16):
    drawn = jax.random.normal(stream_key, extent, jnp.float32) * spread
    if len(pieces) > 0:
        drawn = block_scale(stream_key, extent, pieces, -0.22, 0.18) * drawn
    return jnp.clip(drawn, min=-reach, max=reach).astype(held_as)


def setup_inputs(seed: int = 0, part: int = 0) -> dict:
    streams_of = jax.random.split(jax.random.key(seed), 12)
    part_splits = jax.random.split(jax.random.fold_in(streams_of[11], part), 12)
    return {
        "cells": centred(part_splits[0], (R, F, E), 1.0, 6.0, ((1, 64),)),
        "missing": touch_ends((jax.random.randint(part_splits[1], (R, F), 0, 4) < 1).astype(jnp.int32), jax.random.fold_in(part_splits[1], 1), 0, 1),
        "feat_ids": touch_ends(jax.random.randint(part_splits[2], (F,), 0, NCAT), jax.random.fold_in(part_splits[2], 1), 0, NCAT - 1).astype(jnp.int32),
        "feat_table": centred(streams_of[3], (NCAT, E), 0.7, 5.0, (), jnp.float32),
        "nan_embed": centred(streams_of[4], (E,), 1.0, 5.0, (), jnp.float32),
        "gain_one": jnp.clip(1.0 + 0.18 * jax.random.normal(streams_of[5], (E,), jnp.float32), 0.1, 1.9),
        "w_qkv": draw_w_qkv(jax.random.fold_in(streams_of[11], 71), part),
        "w_out": centred(streams_of[7], (E, E), E ** -0.5, 0.4375),
        "gain_two": jnp.clip(1.0 + 0.18 * jax.random.normal(streams_of[8], (E,), jnp.float32), 0.1, 1.9),
        "w_up": centred(streams_of[9], (E, MLP), E ** -0.5, 0.4375),
        "w_down": centred(streams_of[10], (MLP, E), MLP ** -0.5, 0.21875),
    }


def cell_norm(values, gain):
    mean = lax.optimization_barrier(jnp.mean(values, axis=-1, keepdims=True))
    centered = values - mean
    var = lax.optimization_barrier(jnp.mean(centered * centered, axis=-1, keepdims=True))
    return centered * lax.rsqrt(var + 1e-05) * gain

def attend(qkv):
    width = qkv.shape[-1] // 3
    count = qkv.shape[0]
    head_dim = width // HEADS
    query = qkv[:, :width].reshape(count, HEADS, head_dim).astype(jnp.float32)
    keys = qkv[:, width:2 * width].reshape(count, HEADS, head_dim).astype(jnp.float32)
    values = qkv[:, 2 * width:].reshape(count, HEADS, head_dim).astype(jnp.float32)
    scores = jnp.einsum('qhd,phd->hqp', query, keys) * head_dim ** (-0.5)
    top = lax.optimization_barrier(jnp.max(scores, axis=-1, keepdims=True))
    expo = jnp.exp(scores - top)
    probs = (expo / lax.optimization_barrier(jnp.sum(expo, axis=-1, keepdims=True))).astype(jnp.bfloat16)
    context = jnp.einsum('hqp,phd->qhd', probs.astype(jnp.float32), values)
    return context.astype(jnp.bfloat16).reshape(count, width)

def reference(cells, missing, feat_ids, feat_table, nan_embed, gain_one, w_qkv, w_out, gain_two, w_up, w_down):
    onehot = (feat_ids[:, None] == jnp.arange(NCAT, dtype=jnp.int32)[None, :]).astype(jnp.float32)
    femb = jnp.dot(onehot, feat_table, precision=lax.Precision.HIGHEST)
    tokens = (cells.astype(jnp.float32) + missing[..., None].astype(jnp.float32) * nan_embed + femb[None]).astype(jnp.bfloat16)

    def one_row(row):
        base = row.astype(jnp.float32)
        normed = cell_norm(base, gain_one).astype(jnp.bfloat16)
        qkv = jnp.dot(normed, w_qkv, preferred_element_type=jnp.float32).astype(jnp.bfloat16)
        context = attend(qkv)
        mid = base + jnp.dot(context, w_out, preferred_element_type=jnp.float32)
        normed_two = cell_norm(mid, gain_two).astype(jnp.bfloat16)
        act = jax.nn.gelu(jnp.dot(normed_two, w_up, preferred_element_type=jnp.float32), approximate=False).astype(jnp.bfloat16)
        return mid + jnp.dot(act, w_down, preferred_element_type=jnp.float32)
    return lax.map(one_row, tokens)
```

```python
import functools
import math

import jax
import jax.numpy as jnp
from jax import lax
from jax.experimental import pallas as pl
from jax.experimental.pallas import tpu as pltpu
from jax.sharding import Mesh
from jax.sharding import PartitionSpec as P

HEADS = 6
CORES = 2
LANES = 128
FEAT = ("chip", "core")
MESH = pl.DeviceIdType.MESH


def cell_norm(values, gain):
    mean = jnp.mean(values, axis=-1, keepdims=True)
    centered = values - mean
    var = jnp.mean(centered * centered, axis=-1, keepdims=True)
    return centered * lax.rsqrt(var + 1e-05) * gain


def gelu(x):
    return 0.5 * x * (1.0 + lax.erf(x * math.sqrt(0.5)))


def kernel(
    n,
    phases,
    cells_ref,
    missing_ref,
    ids_ref,
    table_ref,
    nan_ref,
    gain_one_ref,
    w_qkv_ref,
    w_out_ref,
    gain_two_ref,
    w_up_ref,
    w_down_ref,
    out_ref,
    x_ref,
    rx_ref,
    tx_ref,
    y_ref,
    w_ref,
    q_ref,
    k_ref,
    v_ref,
    ctx_ref,
    f_send,
    f_recv,
    kv_send,
    kv_recv,
    b_send,
    b_recv,
):
    me = lax.axis_index("chip")
    core = lax.axis_index("core")
    rows, feats, width = cells_ref.shape
    per_chip = rows // n
    half = n * feats
    rest = width - LANES
    head_dim = width // HEADS

    def chip_at(k):
        return lax.rem(me + k, n)

    barrier = pltpu.get_barrier_semaphore()
    pl.semaphore_signal(barrier, inc=1, device_id={"core": 1 - core}, device_id_type=MESH)
    for k in range(1, n):
        pl.semaphore_signal(barrier, inc=1, device_id={"chip": chip_at(k)}, device_id_type=MESH)

    for i in range(3):
        w_ref[i] = w_qkv_ref[:, i * width : (i + 1) * width]

    spot = lax.broadcasted_iota(jnp.int32, (table_ref.shape[0], feats), 0)
    onehot = (spot == ids_ref[...]).astype(jnp.float32)
    femb = lax.dot_general(
        onehot,
        table_ref[...],
        (((0,), (0,)), ((), ())),
        precision=lax.Precision.HIGHEST,
        preferred_element_type=jnp.float32,
    )
    chips_step = 8 if n % 8 == 0 else n
    step = per_chip * chips_step
    cells_step = step * feats

    def make_tokens(i, carry):
        start = pl.multiple_of(i * step, 8)
        miss = missing_ref[pl.ds(start, step), :].astype(jnp.float32).astype(jnp.bfloat16)
        line = lax.broadcasted_iota(jnp.int32, (cells_step, step), 0)
        column = lax.broadcasted_iota(jnp.int32, (cells_step, step), 1)
        pick = jnp.where(line // feats == column, 1.0, 0.0).astype(jnp.bfloat16)
        spread = jnp.dot(pick, miss, preferred_element_type=jnp.float32)
        line = lax.broadcasted_iota(jnp.int32, (cells_step, feats), 0)
        column = lax.broadcasted_iota(jnp.int32, (cells_step, feats), 1)
        flag = jnp.sum(jnp.where(line % feats == column, spread, 0.0), axis=-1, keepdims=True)
        tokens = (
            cells_ref[pl.ds(start, step)].astype(jnp.float32)
            + (flag * nan_ref[...]).reshape(step, feats, width)
            + femb[None]
        )
        head = tokens[:, :, :LANES].astype(jnp.bfloat16).reshape(chips_step, phases, 2, feats, LANES)
        tail = tokens[:, :, LANES:].reshape(chips_step * phases, 2, feats, rest)
        tail = jnp.concatenate([tail[:, 0], tail[:, 1]], axis=-1).astype(jnp.bfloat16)
        tail = tail.reshape(chips_step, phases, feats, LANES)
        chips = pl.ds(i * chips_step, chips_step)
        for p in range(phases):
            x_ref[p, chips, :feats, :] = head[:, p, 0]
            x_ref[p, chips, feats : 2 * feats, :] = head[:, p, 1]
            x_ref[p, chips, 2 * feats :, :] = tail[:, p]
        return carry

    lax.fori_loop(0, rows // step, make_tokens, 0)
    pl.semaphore_wait(barrier, n)

    def forward(p, k):
        return pltpu.make_async_remote_copy(
            src_ref=x_ref.at[p, chip_at(k)],
            dst_ref=rx_ref.at[p, k],
            send_sem=f_send.at[p],
            recv_sem=f_recv.at[p],
            device_id={"chip": chip_at(k)},
            device_id_type=MESH,
        )

    def backward(p, k):
        return pltpu.make_async_remote_copy(
            src_ref=tx_ref.at[p, k],
            dst_ref=y_ref.at[p, k],
            send_sem=b_send.at[p],
            recv_sem=b_recv.at[p],
            device_id={"chip": chip_at(n - k)},
            device_id_type=MESH,
        )

    def send_all(copy, p):
        copy(p, n // 2).start()

        def pair(i, carry):
            far = n // 2 - 1 - i
            copy(p, far).start()
            copy(p, n - far).start()
            return carry

        lax.fori_loop(0, n // 2 - 1, pair, 0)

    def whole(src, dst, send, recv, p):
        return pltpu.make_async_remote_copy(
            src_ref=src.at[p, pl.ds(1, n - 1)],
            dst_ref=dst.at[p, pl.ds(1, n - 1)],
            send_sem=send.at[p],
            recv_sem=recv.at[p],
            device_id={"chip": chip_at(1)},
            device_id_type=MESH,
        )

    def swap(p, which):
        ref = (k_ref, v_ref)[which]
        return pltpu.make_async_remote_copy(
            src_ref=ref.at[p, :, pl.ds(0, half)],
            dst_ref=ref.at[p, :, pl.ds(half, half)],
            send_sem=kv_send.at[p, which],
            recv_sem=kv_recv.at[p, which],
            device_id={"core": 1 - core},
            device_id_type=MESH,
        )

    lax.fori_loop(0, phases, lambda p, c: (send_all(forward, p), c)[1], 0)

    def base_of(p, r):
        first = rx_ref[p, :, r * feats : (r + 1) * feats, :].astype(jnp.float32).reshape(half, LANES)
        last = rx_ref[p, :, 2 * feats :, :].astype(jnp.float32).reshape(half, LANES)
        return jnp.concatenate([first, last[:, r * rest : (r + 1) * rest]], axis=-1)

    def phase(p, carry):
        rx_ref[p, 0] = x_ref[p, me]
        whole(x_ref, rx_ref, f_send, f_recv, p).wait_recv()
        for r in range(2):
            normed = cell_norm(base_of(p, r), gain_one_ref[...]).astype(jnp.bfloat16)
            for ref, i in ((k_ref, 1), (v_ref, 2)):
                made = jnp.dot(normed, w_ref[i], preferred_element_type=jnp.float32)
                ref[p, r, :half] = made.astype(jnp.bfloat16)
            made = jnp.dot(normed, w_ref[0], preferred_element_type=jnp.float32)
            q_ref[r] = made.astype(jnp.bfloat16)
        for which in range(2):
            swap(p, which).start()
        for which in range(2):
            swap(p, which).wait_recv()

        lane_head = lax.broadcasted_iota(jnp.int32, (half, width), 1) // head_dim
        results = []
        for r in range(2):

            def one_head(h, carry):
                mine = lane_head == h
                query = jnp.where(mine, q_ref[r].astype(jnp.float32), 0.0).astype(jnp.bfloat16)
                scores = lax.dot_general(
                    query, k_ref[p, r], (((1,), (1,)), ((), ())), preferred_element_type=jnp.float32
                )
                top = jnp.max(scores, axis=-1, keepdims=True)
                expo = jnp.exp2((scores - top) * (head_dim**-0.5 * math.log2(math.e)))
                probs = expo * (1.0 / jnp.sum(expo, axis=-1, keepdims=True))
                got = jnp.dot(
                    probs.astype(jnp.bfloat16), v_ref[p, r], preferred_element_type=jnp.float32
                )
                ctx_ref[...] = jnp.where(mine, got.astype(jnp.bfloat16), ctx_ref[...])
                return carry

            lax.fori_loop(0, HEADS, one_head, 0)
            mid = base_of(p, r) + jnp.dot(
                ctx_ref[...], w_out_ref[...], preferred_element_type=jnp.float32
            )
            normed = cell_norm(mid, gain_two_ref[...]).astype(jnp.bfloat16)
            act = gelu(jnp.dot(normed, w_up_ref[...], preferred_element_type=jnp.float32))
            result = mid + jnp.dot(
                act.astype(jnp.bfloat16), w_down_ref[...], preferred_element_type=jnp.float32
            )
            tx_ref[p, :, r * feats : (r + 1) * feats, :] = (
                result[:, :LANES].astype(jnp.bfloat16).reshape(n, feats, LANES)
            )
            results.append(result[:, LANES:])
        tail = jnp.concatenate(results, axis=-1).astype(jnp.bfloat16)
        tx_ref[p, :, 2 * feats :, :] = tail.reshape(n, feats, LANES)
        send_all(backward, p)
        y_ref[p, 0] = tx_ref[p, 0]
        return carry

    lax.fori_loop(0, phases, phase, 0)

    def place(p, carry):
        whole(tx_ref, y_ref, b_send, b_recv, p).wait_recv()

        def one(k, carry):
            row = chip_at(k) * per_chip + 2 * p
            last = y_ref[p, k, 2 * feats :, :]
            for r in range(2):
                first = y_ref[p, k, r * feats : (r + 1) * feats, :]
                out_ref[row + r] = jnp.concatenate(
                    [first, last[:, r * rest : (r + 1) * rest]], axis=-1
                )
            return carry

        lax.fori_loop(0, n, one, 0)
        return carry

    lax.fori_loop(0, phases, place, 0)

    def drain(p, carry):
        whole(x_ref, rx_ref, f_send, f_recv, p).wait_send()
        whole(tx_ref, y_ref, b_send, b_recv, p).wait_send()
        for which in range(2):
            swap(p, which).wait_send()
        return carry

    lax.fori_loop(0, phases, drain, 0)


def solution(mesh):
    groups = mesh.shape["groups"]
    n = mesh.shape["feat"] // CORES
    split = Mesh(mesh.devices.reshape(groups, n, CORES), ("groups", *FEAT))

    def body(
        cells, missing, feat_ids, table, nan_embed, gain_one, w_qkv, w_out, gain_two, w_up, w_down
    ):
        rows, feats, width = cells.shape
        phases = rows // n // 2
        packed = pltpu.VMEM((phases, n, 3 * feats, LANES), jnp.bfloat16)
        half = n * feats
        keys = pltpu.VMEM((phases, 2, CORES * half, width), jnp.bfloat16)
        dma = pltpu.SemaphoreType.DMA
        out = pl.pallas_call(
            functools.partial(kernel, n, phases),
            out_shape=jax.ShapeDtypeStruct(cells.shape, jnp.bfloat16),
            in_specs=[pl.BlockSpec(memory_space=pltpu.VMEM)] * 11,
            out_specs=pl.BlockSpec(memory_space=pltpu.VMEM),
            scratch_shapes=[
                packed,
                packed,
                packed,
                packed,
                pltpu.VMEM((3, width, width), jnp.bfloat16),
                pltpu.VMEM((2, half, width), jnp.bfloat16),
                keys,
                keys,
                pltpu.VMEM((half, width), jnp.bfloat16),
                dma((phases,)),
                dma((phases,)),
                dma((phases, 2)),
                dma((phases, 2)),
                dma((phases,)),
                dma((phases,)),
            ],
            compiler_params=pltpu.CompilerParams(collective_id=0, has_side_effects=True),
        )(
            cells,
            missing,
            feat_ids[None],
            table,
            nan_embed[None],
            gain_one[None],
            w_qkv,
            w_out,
            gain_two[None],
            w_up,
            w_down,
        )
        return out.astype(jnp.float32)

    spread = P("groups", FEAT, None)
    in_specs = (spread, P("groups", FEAT), P(("groups", *FEAT))) + (P(),) * 8
    return jax.shard_map(
        body, mesh=split, in_specs=in_specs, out_specs=spread, check_vma=False
    )
```

```python
import functools
import math

import jax
import jax.numpy as jnp
from jax import lax
from jax.experimental import pallas as pl
from jax.experimental.pallas import tpu as pltpu
from jax.sharding import Mesh
from jax.sharding import PartitionSpec as P

HEADS = 6
CORES = 2
LANES = 128
FEAT = ("chip", "core")
MESH = pl.DeviceIdType.MESH


def cell_norm(values, gain):
    mean = jnp.mean(values, axis=-1, keepdims=True)
    centered = values - mean
    var = jnp.mean(centered * centered, axis=-1, keepdims=True)
    return centered * lax.rsqrt(var + 1e-05) * gain


def gelu(x):
    return 0.5 * x * (1.0 + lax.erf(x * math.sqrt(0.5)))


def kernel(
    n,
    phases,
    cells_hbm,
    missing_hbm,
    ids_hbm,
    table_hbm,
    nan_hbm,
    gain_one_hbm,
    w_qkv_hbm,
    w_out_hbm,
    gain_two_hbm,
    w_up_hbm,
    w_down_hbm,
    y_ref,
    cells_ref,
    missing_ref,
    ids_ref,
    table_ref,
    nan_ref,
    gain_one_ref,
    w_qkv_ref,
    w_out_ref,
    gain_two_ref,
    w_up_ref,
    w_down_ref,
    x_ref,
    rx_ref,
    tx_ref,
    w_ref,
    q_ref,
    k_ref,
    v_ref,
    ctx_ref,
    c_sem,
    in_sem,
    own_sem,
    f_send,
    f_recv,
    kv_send,
    kv_recv,
    b_send,
    b_recv,
):
    me = lax.axis_index("chip")
    core = lax.axis_index("core")
    feats, width = cells_ref.shape[3:]
    per_chip = 2 * phases
    rows = n * per_chip
    half = n * feats
    rest = width - LANES
    head_dim = width // HEADS

    def chip_at(k):
        return lax.rem(me + k, n)

    barrier = pltpu.get_barrier_semaphore()
    pl.semaphore_signal(barrier, inc=1, device_id={"core": 1 - core}, device_id_type=MESH)
    for k in range(1, n):
        pl.semaphore_signal(barrier, inc=1, device_id={"chip": chip_at(k)}, device_id_type=MESH)

    first = [
        (missing_hbm, missing_ref),
        (ids_hbm, ids_ref),
        (table_hbm, table_ref),
        (nan_hbm, nan_ref),
    ]
    later = [
        (gain_one_hbm, gain_one_ref),
        (w_qkv_hbm, w_qkv_ref),
        (w_out_hbm, w_out_ref),
        (gain_two_hbm, gain_two_ref),
        (w_up_hbm, w_up_ref),
        (w_down_hbm, w_down_ref),
    ]
    loads = [
        pltpu.make_async_copy(src, dst, in_sem.at[i]) for i, (src, dst) in enumerate(first + later)
    ]
    cell_loads = [
        pltpu.make_async_copy(cells_hbm.at[:, p], cells_ref.at[p], c_sem.at[p])
        for p in range(phases)
    ]
    for load in loads[: len(first)] + cell_loads + loads[len(first) :]:
        load.start()
    for load in loads[: len(first)]:
        load.wait()

    spot = lax.broadcasted_iota(jnp.int32, (table_ref.shape[0], feats), 0)
    onehot = (spot == ids_ref[...]).astype(jnp.float32)
    femb = lax.dot_general(
        onehot,
        table_ref[...],
        (((0,), (0,)), ((), ())),
        precision=lax.Precision.HIGHEST,
        preferred_element_type=jnp.float32,
    )
    miss = missing_ref[...].astype(jnp.float32).astype(jnp.bfloat16)
    count = n * 2 * feats

    def make_tokens(p):
        line = lax.broadcasted_iota(jnp.int32, (count, rows), 0) // feats
        column = lax.broadcasted_iota(jnp.int32, (count, rows), 1)
        row = (line // 2) * per_chip + 2 * p + line % 2
        pick = jnp.where(row == column, 1.0, 0.0).astype(jnp.bfloat16)
        spread = lax.dot_general(
            pick, miss, (((1,), (1,)), ((), ())), preferred_element_type=jnp.float32
        )
        line = lax.broadcasted_iota(jnp.int32, (count, feats), 0)
        column = lax.broadcasted_iota(jnp.int32, (count, feats), 1)
        flag = jnp.sum(jnp.where(line % feats == column, spread, 0.0), axis=-1, keepdims=True)
        cell_loads[p].wait()
        tokens = (
            cells_ref[p].astype(jnp.float32)
            + (flag * nan_ref[...]).reshape(n, 2, feats, width)
            + femb[None, None]
        )
        for r in range(2):
            x_ref[p, :, r * feats : (r + 1) * feats, :] = tokens[:, r, :, :LANES].astype(jnp.bfloat16)
        tail = jnp.concatenate([tokens[:, 0, :, LANES:], tokens[:, 1, :, LANES:]], axis=-1)
        x_ref[p, :, 2 * feats :, :] = tail.astype(jnp.bfloat16)

    def forward(p, k):
        return pltpu.make_async_remote_copy(
            src_ref=x_ref.at[p, chip_at(k)],
            dst_ref=rx_ref.at[p, k],
            send_sem=f_send.at[p],
            recv_sem=f_recv.at[p],
            device_id={"chip": chip_at(k)},
            device_id_type=MESH,
        )

    def backward(p, k):
        return pltpu.make_async_remote_copy(
            src_ref=tx_ref.at[p, k],
            dst_ref=y_ref.at[p, me],
            send_sem=b_send.at[p],
            recv_sem=b_recv.at[p],
            device_id={"chip": chip_at(n - k)},
            device_id_type=MESH,
        )

    def send_all(copy, p):
        copy(p, n // 2).start()

        def pair(i, carry):
            far = n // 2 - 1 - i
            copy(p, far).start()
            copy(p, n - far).start()
            return carry

        lax.fori_loop(0, n // 2 - 1, pair, 0)

    def whole(src, dst, send, recv, p):
        return pltpu.make_async_remote_copy(
            src_ref=src.at[p, pl.ds(1, n - 1)],
            dst_ref=dst.at[p, pl.ds(1, n - 1)],
            send_sem=send.at[p],
            recv_sem=recv.at[p],
            device_id={"chip": chip_at(1)},
            device_id_type=MESH,
        )

    def swap(p, which):
        ref = (k_ref, v_ref)[which]
        return pltpu.make_async_remote_copy(
            src_ref=ref.at[p, :, pl.ds(0, half)],
            dst_ref=ref.at[p, :, pl.ds(half, half)],
            send_sem=kv_send.at[p, which],
            recv_sem=kv_recv.at[p, which],
            device_id={"core": 1 - core},
            device_id_type=MESH,
        )

    for p in range(phases):
        make_tokens(p)
        if p == 0:
            pl.semaphore_wait(barrier, n)
        send_all(forward, p)

    for load in loads[len(first) :]:
        load.wait()
    for i in range(3):
        w_ref[i] = w_qkv_ref[:, i * width : (i + 1) * width]

    def own(p):
        return pltpu.make_async_copy(tx_ref.at[p, 0], y_ref.at[p, me], own_sem.at[p])

    def base_of(p, r):
        first = rx_ref[p, :, r * feats : (r + 1) * feats, :].astype(jnp.float32).reshape(half, LANES)
        last = rx_ref[p, :, 2 * feats :, :].astype(jnp.float32).reshape(half, LANES)
        return jnp.concatenate([first, last[:, r * rest : (r + 1) * rest]], axis=-1)

    def phase(p, carry):
        rx_ref[p, 0] = x_ref[p, me]
        whole(x_ref, rx_ref, f_send, f_recv, p).wait_recv()
        for r in range(2):
            normed = cell_norm(base_of(p, r), gain_one_ref[...]).astype(jnp.bfloat16)
            for ref, i in ((k_ref, 1), (v_ref, 2)):
                made = jnp.dot(normed, w_ref[i], preferred_element_type=jnp.float32)
                ref[p, r, :half] = made.astype(jnp.bfloat16)
            made = jnp.dot(normed, w_ref[0], preferred_element_type=jnp.float32)
            q_ref[r] = made.astype(jnp.bfloat16)
        for which in range(2):
            swap(p, which).start()
        for which in range(2):
            swap(p, which).wait_recv()

        lane_head = lax.broadcasted_iota(jnp.int32, (half, width), 1) // head_dim
        results = []
        for r in range(2):

            def one_head(h, carry):
                mine = lane_head == h
                query = jnp.where(mine, q_ref[r].astype(jnp.float32), 0.0).astype(jnp.bfloat16)
                scores = lax.dot_general(
                    query, k_ref[p, r], (((1,), (1,)), ((), ())), preferred_element_type=jnp.float32
                )
                top = jnp.max(scores, axis=-1, keepdims=True)
                expo = jnp.exp2((scores - top) * (head_dim**-0.5 * math.log2(math.e)))
                probs = expo * (1.0 / jnp.sum(expo, axis=-1, keepdims=True))
                got = jnp.dot(
                    probs.astype(jnp.bfloat16), v_ref[p, r], preferred_element_type=jnp.float32
                )
                ctx_ref[...] = jnp.where(mine, got.astype(jnp.bfloat16), ctx_ref[...])
                return carry

            lax.fori_loop(0, HEADS, one_head, 0)
            mid = base_of(p, r) + jnp.dot(
                ctx_ref[...], w_out_ref[...], preferred_element_type=jnp.float32
            )
            normed = cell_norm(mid, gain_two_ref[...]).astype(jnp.bfloat16)
            act = gelu(jnp.dot(normed, w_up_ref[...], preferred_element_type=jnp.float32))
            result = mid + lax.dot_general(
                act.astype(jnp.bfloat16),
                w_down_ref[...],
                (((1,), (1,)), ((), ())),
                preferred_element_type=jnp.float32,
            )
            tx_ref[p, :, r * feats : (r + 1) * feats, :] = (
                result[:, :LANES].astype(jnp.bfloat16).reshape(n, feats, LANES)
            )
            results.append(result[:, LANES:])
        tail = jnp.concatenate(results, axis=-1).astype(jnp.bfloat16)
        tx_ref[p, :, 2 * feats :, :] = tail.reshape(n, feats, LANES)
        send_all(backward, p)
        own(p).start()
        return carry

    lax.fori_loop(0, phases, phase, 0)

    def drain(p, carry):
        whole(tx_ref, y_ref, b_send, b_recv, p).wait_recv()
        own(p).wait()
        whole(x_ref, rx_ref, f_send, f_recv, p).wait_send()
        whole(tx_ref, y_ref, b_send, b_recv, p).wait_send()
        for which in range(2):
            swap(p, which).wait_send()
        return carry

    lax.fori_loop(0, phases, drain, 0)


def unpack(y_ref, out_ref):
    phases = out_ref.shape[1]
    feats, width = out_ref.shape[3:]
    rest = width - LANES
    for p in range(phases):
        last = y_ref[p, :, 2 * feats :, :].astype(jnp.float32)
        for r in range(2):
            first = y_ref[p, :, r * feats : (r + 1) * feats, :].astype(jnp.float32)
            out_ref[:, p, r, :, :LANES] = first
            out_ref[:, p, r, :, LANES:] = last[:, :, r * rest : (r + 1) * rest]


def solution(mesh):
    groups = mesh.shape["groups"]
    n = mesh.shape["feat"] // CORES
    split = Mesh(mesh.devices.reshape(groups, n, CORES), ("groups", *FEAT))

    def body(
        cells, missing, feat_ids, table, nan_embed, gain_one, w_qkv, w_out, gain_two, w_up, w_down
    ):
        rows, feats, width = cells.shape
        phases = rows // n // 2
        packed = pltpu.VMEM((phases, n, 3 * feats, LANES), jnp.bfloat16)
        half = n * feats
        keys = pltpu.VMEM((phases, 2, CORES * half, width), jnp.bfloat16)
        dma = pltpu.SemaphoreType.DMA
        vmem = pltpu.VMEM
        anywhere = pl.BlockSpec(memory_space=pl.ANY)
        y = pl.pallas_call(
            functools.partial(kernel, n, phases),
            out_shape=jax.ShapeDtypeStruct(packed.shape, jnp.bfloat16),
            in_specs=[anywhere] * 11,
            out_specs=anywhere,
            scratch_shapes=[
                vmem((phases, n, 2, feats, width), cells.dtype),
                vmem((feats, rows), missing.dtype),
                vmem((1, feats), feat_ids.dtype),
                vmem(table.shape, table.dtype),
                vmem((1, width), nan_embed.dtype),
                vmem((1, width), gain_one.dtype),
                vmem(w_qkv.shape, w_qkv.dtype),
                vmem(w_out.shape, w_out.dtype),
                vmem((1, width), gain_two.dtype),
                vmem(w_up.shape, w_up.dtype),
                vmem(w_down.shape[::-1], w_down.dtype),
                packed,
                packed,
                packed,
                vmem((3, width, width), jnp.bfloat16),
                vmem((2, half, width), jnp.bfloat16),
                keys,
                keys,
                vmem((half, width), jnp.bfloat16),
                dma((phases,)),
                dma((10,)),
                dma((phases,)),
                dma((phases,)),
                dma((phases,)),
                dma((phases, 2)),
                dma((phases, 2)),
                dma((phases,)),
                dma((phases,)),
            ],
            compiler_params=pltpu.CompilerParams(collective_id=0, has_side_effects=True),
        )(
            cells.reshape(n, phases, 2, feats, width),
            missing.T,
            feat_ids[None],
            table,
            nan_embed[None],
            gain_one[None],
            w_qkv,
            w_out,
            gain_two[None],
            w_up,
            w_down.T,
        )
        steps = 4 if n % 4 == 0 else 1
        out = pl.pallas_call(
            unpack,
            grid=(steps,),
            out_shape=jax.ShapeDtypeStruct((n, phases, 2, feats, width), jnp.float32),
            in_specs=[pl.BlockSpec((phases, n // steps, 3 * feats, LANES), lambda i: (0, i, 0, 0))],
            out_specs=pl.BlockSpec((n // steps, phases, 2, feats, width), lambda i: (i, 0, 0, 0, 0)),
        )(y)
        return out.reshape(rows, feats, width)

    spread = P("groups", FEAT, None)
    in_specs = (spread, P("groups", FEAT), P(("groups", *FEAT))) + (P(),) * 8
    return jax.shard_map(
        body, mesh=split, in_specs=in_specs, out_specs=spread, check_vma=False
    )
```

```python
import functools
import math

import jax
import jax.numpy as jnp
from jax import lax
from jax.experimental import pallas as pl
from jax.experimental.pallas import tpu as pltpu
from jax.sharding import Mesh
from jax.sharding import PartitionSpec as P

HEADS = 6
CORES = 2
LANES = 128
FEAT = ("chip", "core")
MESH = pl.DeviceIdType.MESH


def cell_norm(values, gain):
    mean = jnp.mean(values, axis=-1, keepdims=True)
    centered = values - mean
    var = jnp.mean(centered * centered, axis=-1, keepdims=True)
    return centered * lax.rsqrt(var + 1e-05) * gain


def gelu(x):
    return 0.5 * x * (1.0 + lax.erf(x * math.sqrt(0.5)))


def kernel(
    n,
    phases,
    cells_hbm,
    missing_hbm,
    ids_hbm,
    table_hbm,
    nan_hbm,
    gain_one_hbm,
    w_qkv_hbm,
    w_out_hbm,
    gain_two_hbm,
    w_up_hbm,
    w_down_hbm,
    y_ref,
    cells_ref,
    missing_ref,
    ids_ref,
    table_ref,
    nan_ref,
    gain_one_ref,
    w_qkv_ref,
    w_out_ref,
    gain_two_ref,
    w_up_ref,
    w_down_ref,
    x_ref,
    rx_ref,
    tx_ref,
    w_ref,
    q_ref,
    k_ref,
    v_ref,
    ctx_ref,
    c_sem,
    in_sem,
    own_sem,
    f_send,
    f_recv,
    kv_send,
    kv_recv,
    b_send,
    b_recv,
):
    me = lax.axis_index("chip")
    core = lax.axis_index("core")
    feats, width = cells_ref.shape[3:]
    per_chip = 2 * phases
    rows = n * per_chip
    half = n * feats
    rest = width - LANES
    head_dim = width // HEADS

    def chip_at(k):
        return lax.rem(me + k, n)

    barrier = pltpu.get_barrier_semaphore()
    pl.semaphore_signal(barrier, inc=1, device_id={"core": 1 - core}, device_id_type=MESH)
    for k in range(1, n):
        pl.semaphore_signal(barrier, inc=1, device_id={"chip": chip_at(k)}, device_id_type=MESH)

    first = [
        (missing_hbm, missing_ref),
        (ids_hbm, ids_ref),
        (table_hbm, table_ref),
        (nan_hbm, nan_ref),
    ]
    later = [
        (gain_one_hbm, gain_one_ref),
        (w_qkv_hbm, w_qkv_ref),
        (w_out_hbm, w_out_ref),
        (gain_two_hbm, gain_two_ref),
        (w_up_hbm, w_up_ref),
        (w_down_hbm, w_down_ref),
    ]
    loads = [
        pltpu.make_async_copy(src, dst, in_sem.at[i]) for i, (src, dst) in enumerate(first + later)
    ]
    cell_loads = [
        pltpu.make_async_copy(cells_hbm.at[:, p], cells_ref.at[p], c_sem.at[p])
        for p in range(phases)
    ]
    for load in loads[: len(first)] + cell_loads + loads[len(first) :]:
        load.start()
    for load in loads[: len(first)]:
        load.wait()

    spot = lax.broadcasted_iota(jnp.int32, (table_ref.shape[0], feats), 0)
    onehot = (spot == ids_ref[...]).astype(jnp.float32)
    femb = lax.dot_general(
        onehot,
        table_ref[...],
        (((0,), (0,)), ((), ())),
        precision=lax.Precision.HIGHEST,
        preferred_element_type=jnp.float32,
    )
    miss = missing_ref[...].astype(jnp.float32).astype(jnp.bfloat16)
    count = n * 2 * feats

    def make_tokens(p):
        line = lax.broadcasted_iota(jnp.int32, (count, rows), 0) // feats
        column = lax.broadcasted_iota(jnp.int32, (count, rows), 1)
        row = (line // 2) * per_chip + 2 * p + line % 2
        pick = jnp.where(row == column, 1.0, 0.0).astype(jnp.bfloat16)
        spread = lax.dot_general(
            pick, miss, (((1,), (1,)), ((), ())), preferred_element_type=jnp.float32
        )
        line = lax.broadcasted_iota(jnp.int32, (count, feats), 0)
        column = lax.broadcasted_iota(jnp.int32, (count, feats), 1)
        flag = jnp.sum(jnp.where(line % feats == column, spread, 0.0), axis=-1, keepdims=True)
        cell_loads[p].wait()
        tokens = (
            cells_ref[p].astype(jnp.float32)
            + (flag * nan_ref[...]).reshape(n, 2, feats, width)
            + femb[None, None]
        )
        for r in range(2):
            x_ref[p, :, r * feats : (r + 1) * feats, :] = tokens[:, r, :, :LANES].astype(jnp.bfloat16)
        tail = jnp.concatenate([tokens[:, 0, :, LANES:], tokens[:, 1, :, LANES:]], axis=-1)
        x_ref[p, :, 2 * feats :, :] = tail.astype(jnp.bfloat16)

    def forward(p, k):
        return pltpu.make_async_remote_copy(
            src_ref=x_ref.at[p, chip_at(k)],
            dst_ref=rx_ref.at[p, k],
            send_sem=f_send.at[p],
            recv_sem=f_recv.at[p],
            device_id={"chip": chip_at(k)},
            device_id_type=MESH,
        )

    def backward(p, k):
        return pltpu.make_async_remote_copy(
            src_ref=tx_ref.at[p, k],
            dst_ref=y_ref.at[p, me],
            send_sem=b_send.at[p],
            recv_sem=b_recv.at[p],
            device_id={"chip": chip_at(n - k)},
            device_id_type=MESH,
        )

    def send_all(copy, p):
        copy(p, n // 2).start()

        def pair(i, carry):
            far = n // 2 - 1 - i
            copy(p, far).start()
            copy(p, n - far).start()
            return carry

        lax.fori_loop(0, n // 2 - 1, pair, 0)

    def send_to(low, high, *which):
        def one(t, carry):
            @pl.when(t != me)
            def _():
                for p in which:
                    backward(p, lax.rem(me + n - t, n)).start()

            return carry

        lax.fori_loop(low, high, one, 0)

    def whole(src, dst, send, recv, p):
        return pltpu.make_async_remote_copy(
            src_ref=src.at[p, pl.ds(1, n - 1)],
            dst_ref=dst.at[p, pl.ds(1, n - 1)],
            send_sem=send.at[p],
            recv_sem=recv.at[p],
            device_id={"chip": chip_at(1)},
            device_id_type=MESH,
        )

    def swap(p, which):
        ref = (k_ref, v_ref)[which]
        return pltpu.make_async_remote_copy(
            src_ref=ref.at[p, :, pl.ds(0, half)],
            dst_ref=ref.at[p, :, pl.ds(half, half)],
            send_sem=kv_send.at[p, which],
            recv_sem=kv_recv.at[p, which],
            device_id={"core": 1 - core},
            device_id_type=MESH,
        )

    for p in range(phases):
        make_tokens(p)
        if p == 0:
            pl.semaphore_wait(barrier, n)
        send_all(forward, p)

    for load in loads[len(first) :]:
        load.wait()
    for i in range(3):
        w_ref[i] = w_qkv_ref[:, i * width : (i + 1) * width]

    def own(p):
        return pltpu.make_async_copy(tx_ref.at[p, 0], y_ref.at[p, me], own_sem.at[p])

    def base_of(p, r):
        first = rx_ref[p, :, r * feats : (r + 1) * feats, :].astype(jnp.float32).reshape(half, LANES)
        last = rx_ref[p, :, 2 * feats :, :].astype(jnp.float32).reshape(half, LANES)
        return jnp.concatenate([first, last[:, r * rest : (r + 1) * rest]], axis=-1)

    def phase(p, carry):
        rx_ref[p, 0] = x_ref[p, me]
        whole(x_ref, rx_ref, f_send, f_recv, p).wait_recv()
        for r in range(2):
            normed = cell_norm(base_of(p, r), gain_one_ref[...]).astype(jnp.bfloat16)
            for ref, i in ((k_ref, 1), (v_ref, 2)):
                made = jnp.dot(normed, w_ref[i], preferred_element_type=jnp.float32)
                ref[p, r, :half] = made.astype(jnp.bfloat16)
            made = jnp.dot(normed, w_ref[0], preferred_element_type=jnp.float32)
            q_ref[r] = made.astype(jnp.bfloat16)
        for which in range(2):
            swap(p, which).start()
        for which in range(2):
            swap(p, which).wait_recv()

        lane_head = lax.broadcasted_iota(jnp.int32, (half, width), 1) // head_dim
        results = []
        for r in range(2):

            def one_head(h, carry):
                mine = lane_head == h
                query = jnp.where(mine, q_ref[r].astype(jnp.float32), 0.0).astype(jnp.bfloat16)
                scores = lax.dot_general(
                    query, k_ref[p, r], (((1,), (1,)), ((), ())), preferred_element_type=jnp.float32
                )
                top = jnp.max(scores, axis=-1, keepdims=True)
                expo = jnp.exp2((scores - top) * (head_dim**-0.5 * math.log2(math.e)))
                probs = expo * (1.0 / jnp.sum(expo, axis=-1, keepdims=True))
                got = jnp.dot(
                    probs.astype(jnp.bfloat16), v_ref[p, r], preferred_element_type=jnp.float32
                )
                ctx_ref[...] = jnp.where(mine, got.astype(jnp.bfloat16), ctx_ref[...])
                return carry

            lax.fori_loop(0, HEADS, one_head, 0)
            mid = base_of(p, r) + jnp.dot(
                ctx_ref[...], w_out_ref[...], preferred_element_type=jnp.float32
            )
            normed = cell_norm(mid, gain_two_ref[...]).astype(jnp.bfloat16)
            act = gelu(jnp.dot(normed, w_up_ref[...], preferred_element_type=jnp.float32))
            result = mid + lax.dot_general(
                act.astype(jnp.bfloat16),
                w_down_ref[...],
                (((1,), (1,)), ((), ())),
                preferred_element_type=jnp.float32,
            )
            tx_ref[p, :, r * feats : (r + 1) * feats, :] = (
                result[:, :LANES].astype(jnp.bfloat16).reshape(n, feats, LANES)
            )
            results.append(result[:, LANES:])
        tail = jnp.concatenate(results, axis=-1).astype(jnp.bfloat16)
        tx_ref[p, :, 2 * feats :, :] = tail.reshape(n, feats, LANES)

        @pl.when(p == 0)
        def _():
            send_to(0, n, p)

        own(p).start()
        return carry

    lax.fori_loop(0, phases, phase, 0)
    send_to(0, n, 1, 2)

    def drain(p, carry):
        whole(tx_ref, y_ref, b_send, b_recv, p).wait_recv()
        own(p).wait()
        whole(x_ref, rx_ref, f_send, f_recv, p).wait_send()
        whole(tx_ref, y_ref, b_send, b_recv, p).wait_send()
        for which in range(2):
            swap(p, which).wait_send()
        return carry

    lax.fori_loop(0, phases, drain, 0)


def unpack(y_ref, out_ref):
    phases = out_ref.shape[1]
    feats, width = out_ref.shape[3:]
    rest = width - LANES
    for p in range(phases):
        last = y_ref[p, :, 2 * feats :, :].astype(jnp.float32)
        for r in range(2):
            first = y_ref[p, :, r * feats : (r + 1) * feats, :].astype(jnp.float32)
            out_ref[:, p, r, :, :LANES] = first
            out_ref[:, p, r, :, LANES:] = last[:, :, r * rest : (r + 1) * rest]


def solution(mesh):
    groups = mesh.shape["groups"]
    n = mesh.shape["feat"] // CORES
    split = Mesh(mesh.devices.reshape(groups, n, CORES), ("groups", *FEAT))

    def body(
        cells, missing, feat_ids, table, nan_embed, gain_one, w_qkv, w_out, gain_two, w_up, w_down
    ):
        rows, feats, width = cells.shape
        phases = rows // n // 2
        packed = pltpu.VMEM((phases, n, 3 * feats, LANES), jnp.bfloat16)
        half = n * feats
        keys = pltpu.VMEM((phases, 2, CORES * half, width), jnp.bfloat16)
        dma = pltpu.SemaphoreType.DMA
        vmem = pltpu.VMEM
        anywhere = pl.BlockSpec(memory_space=pl.ANY)
        y = pl.pallas_call(
            functools.partial(kernel, n, phases),
            out_shape=jax.ShapeDtypeStruct(packed.shape, jnp.bfloat16),
            in_specs=[anywhere] * 11,
            out_specs=anywhere,
            scratch_shapes=[
                vmem((phases, n, 2, feats, width), cells.dtype),
                vmem((feats, rows), missing.dtype),
                vmem((1, feats), feat_ids.dtype),
                vmem(table.shape, table.dtype),
                vmem((1, width), nan_embed.dtype),
                vmem((1, width), gain_one.dtype),
                vmem(w_qkv.shape, w_qkv.dtype),
                vmem(w_out.shape, w_out.dtype),
                vmem((1, width), gain_two.dtype),
                vmem(w_up.shape, w_up.dtype),
                vmem(w_down.shape[::-1], w_down.dtype),
                packed,
                packed,
                packed,
                vmem((3, width, width), jnp.bfloat16),
                vmem((2, half, width), jnp.bfloat16),
                keys,
                keys,
                vmem((half, width), jnp.bfloat16),
                dma((phases,)),
                dma((10,)),
                dma((phases,)),
                dma((phases,)),
                dma((phases,)),
                dma((phases, 2)),
                dma((phases, 2)),
                dma((phases,)),
                dma((phases,)),
            ],
            compiler_params=pltpu.CompilerParams(collective_id=0, has_side_effects=True),
        )(
            cells.reshape(n, phases, 2, feats, width),
            missing.T,
            feat_ids[None],
            table,
            nan_embed[None],
            gain_one[None],
            w_qkv,
            w_out,
            gain_two[None],
            w_up,
            w_down.T,
        )
        steps = 4 if n % 4 == 0 else 1
        out = pl.pallas_call(
            unpack,
            grid=(steps,),
            out_shape=jax.ShapeDtypeStruct((n, phases, 2, feats, width), jnp.float32),
            in_specs=[pl.BlockSpec((phases, n // steps, 3 * feats, LANES), lambda i: (0, i, 0, 0))],
            out_specs=pl.BlockSpec((n // steps, phases, 2, feats, width), lambda i: (i, 0, 0, 0, 0)),
        )(y)
        return out.reshape(rows, feats, width)

    spread = P("groups", FEAT, None)
    in_specs = (spread, P("groups", FEAT), P(("groups", *FEAT))) + (P(),) * 8
    return jax.shard_map(
        body, mesh=split, in_specs=in_specs, out_specs=spread, check_vma=False
    )
```

```python
import functools
import math

import jax
import jax.numpy as jnp
from jax import lax
from jax.experimental import pallas as pl
from jax.experimental.pallas import tpu as pltpu
from jax.sharding import Mesh
from jax.sharding import PartitionSpec as P

HEADS = 6
CORES = 2
LANES = 128
FEAT = ("chip", "core")
MESH = pl.DeviceIdType.MESH


def cell_norm(values, gain):
    mean = jnp.mean(values, axis=-1, keepdims=True)
    centered = values - mean
    var = jnp.mean(centered * centered, axis=-1, keepdims=True)
    return centered * lax.rsqrt(var + 1e-05) * gain


def gelu(x):
    return 0.5 * x * (1.0 + lax.erf(x * math.sqrt(0.5)))


def kernel(
    n,
    phases,
    cells_hbm,
    missing_hbm,
    ids_hbm,
    table_hbm,
    nan_hbm,
    gain_one_hbm,
    w_qkv_hbm,
    w_out_hbm,
    gain_two_hbm,
    w_up_hbm,
    w_down_hbm,
    y_ref,
    cells_ref,
    missing_ref,
    ids_ref,
    table_ref,
    nan_ref,
    gain_one_ref,
    w_qkv_ref,
    w_out_ref,
    gain_two_ref,
    w_up_ref,
    w_down_ref,
    x_ref,
    rx_ref,
    tx_ref,
    w_ref,
    q_ref,
    k_ref,
    v_ref,
    ctx_ref,
    c_sem,
    in_sem,
    own_sem,
    heard,
    f_send,
    f_recv,
    kv_send,
    kv_recv,
    b_send,
    b_recv,
):
    me = lax.axis_index("chip")
    core = lax.axis_index("core")
    feats, width = cells_ref.shape[3:]
    per_chip = 2 * phases
    rows = n * per_chip
    half = n * feats
    rest = width - LANES
    head_dim = width // HEADS

    def chip_at(k):
        return lax.rem(me + k, n)

    near = n // 4
    barrier = pltpu.get_barrier_semaphore()
    pl.semaphore_signal(barrier, inc=1, device_id={"core": 1 - core}, device_id_type=MESH)
    for k in range(1, n):
        ear = 0 if min(k, n - k) <= near else 1
        pl.semaphore_signal(
            barrier, inc=1, device_id={"chip": chip_at(k), "core": ear}, device_id_type=MESH
        )

    def meet(which, count):
        @pl.when(core == which)
        def _():
            pl.semaphore_wait(barrier, CORES * count + 1)
            pl.semaphore_signal(heard, inc=1, device_id={"core": 1 - core}, device_id_type=MESH)

    def hear(which):
        @pl.when(core != which)
        def _():
            pl.semaphore_wait(heard, 1)

    first = [
        (missing_hbm, missing_ref),
        (ids_hbm, ids_ref),
        (table_hbm, table_ref),
        (nan_hbm, nan_ref),
    ]
    later = [
        (gain_one_hbm, gain_one_ref),
        (w_qkv_hbm, w_qkv_ref),
        (w_out_hbm, w_out_ref),
        (gain_two_hbm, gain_two_ref),
        (w_up_hbm, w_up_ref),
        (w_down_hbm, w_down_ref),
    ]
    loads = [
        pltpu.make_async_copy(src, dst, in_sem.at[i]) for i, (src, dst) in enumerate(first + later)
    ]
    cell_loads = [
        pltpu.make_async_copy(cells_hbm.at[:, p], cells_ref.at[p], c_sem.at[p])
        for p in range(phases)
    ]
    for load in loads[: len(first)] + cell_loads + loads[len(first) :]:
        load.start()
    for load in loads[: len(first)]:
        load.wait()

    spot = lax.broadcasted_iota(jnp.int32, (table_ref.shape[0], feats), 0)
    onehot = (spot == ids_ref[...]).astype(jnp.float32)
    femb = lax.dot_general(
        onehot,
        table_ref[...],
        (((0,), (0,)), ((), ())),
        precision=lax.Precision.HIGHEST,
        preferred_element_type=jnp.float32,
    )
    miss = missing_ref[...].astype(jnp.float32).astype(jnp.bfloat16)
    count = n * 2 * feats

    def make_tokens(p):
        line = lax.broadcasted_iota(jnp.int32, (count, rows), 0) // feats
        column = lax.broadcasted_iota(jnp.int32, (count, rows), 1)
        row = (line // 2) * per_chip + 2 * p + line % 2
        pick = jnp.where(row == column, 1.0, 0.0).astype(jnp.bfloat16)
        spread = lax.dot_general(
            pick, miss, (((1,), (1,)), ((), ())), preferred_element_type=jnp.float32
        )
        line = lax.broadcasted_iota(jnp.int32, (count, feats), 0)
        column = lax.broadcasted_iota(jnp.int32, (count, feats), 1)
        flag = jnp.sum(jnp.where(line % feats == column, spread, 0.0), axis=-1, keepdims=True)
        cell_loads[p].wait()
        tokens = (
            cells_ref[p].astype(jnp.float32)
            + (flag * nan_ref[...]).reshape(n, 2, feats, width)
            + femb[None, None]
        )
        for r in range(2):
            x_ref[p, :, r * feats : (r + 1) * feats, :] = tokens[:, r, :, :LANES].astype(jnp.bfloat16)
        tail = jnp.concatenate([tokens[:, 0, :, LANES:], tokens[:, 1, :, LANES:]], axis=-1)
        x_ref[p, :, 2 * feats :, :] = tail.astype(jnp.bfloat16)

    def forward(p, k):
        return pltpu.make_async_remote_copy(
            src_ref=x_ref.at[p, chip_at(k)],
            dst_ref=rx_ref.at[p, k],
            send_sem=f_send.at[p],
            recv_sem=f_recv.at[p],
            device_id={"chip": chip_at(k)},
            device_id_type=MESH,
        )

    def backward(p, k):
        return pltpu.make_async_remote_copy(
            src_ref=tx_ref.at[p, k],
            dst_ref=y_ref.at[p, me],
            send_sem=b_send.at[p],
            recv_sem=b_recv.at[p],
            device_id={"chip": chip_at(n - k)},
            device_id_type=MESH,
        )

    def send_pairs(copy, p, low, high):
        def pair(i, carry):
            copy(p, high - i).start()
            copy(p, n - high + i).start()
            return carry

        lax.fori_loop(0, high - low + 1, pair, 0)

    def send_to(low, high, *which):
        def one(t, carry):
            @pl.when(t != me)
            def _():
                for p in which:
                    backward(p, lax.rem(me + n - t, n)).start()

            return carry

        lax.fori_loop(low, high, one, 0)

    def whole(src, dst, send, recv, p):
        return pltpu.make_async_remote_copy(
            src_ref=src.at[p, pl.ds(1, n - 1)],
            dst_ref=dst.at[p, pl.ds(1, n - 1)],
            send_sem=send.at[p],
            recv_sem=recv.at[p],
            device_id={"chip": chip_at(1)},
            device_id_type=MESH,
        )

    def swap(p, which):
        ref = (k_ref, v_ref)[which]
        return pltpu.make_async_remote_copy(
            src_ref=ref.at[p, :, pl.ds(0, half)],
            dst_ref=ref.at[p, :, pl.ds(half, half)],
            send_sem=kv_send.at[p, which],
            recv_sem=kv_recv.at[p, which],
            device_id={"core": 1 - core},
            device_id_type=MESH,
        )

    make_tokens(0)
    meet(0, 2 * near)
    hear(0)
    for p in range(phases):
        if p > 0:
            make_tokens(p)
        send_pairs(forward, p, 1, near)
    meet(1, n - 1 - 2 * near)
    hear(1)
    for p in range(phases):
        forward(p, n // 2).start()
        send_pairs(forward, p, near + 1, n // 2 - 1)

    for load in loads[len(first) :]:
        load.wait()
    for i in range(3):
        w_ref[i] = w_qkv_ref[:, i * width : (i + 1) * width]

    def own(p):
        return pltpu.make_async_copy(tx_ref.at[p, 0], y_ref.at[p, me], own_sem.at[p])

    def base_of(p, r):
        first = rx_ref[p, :, r * feats : (r + 1) * feats, :].astype(jnp.float32).reshape(half, LANES)
        last = rx_ref[p, :, 2 * feats :, :].astype(jnp.float32).reshape(half, LANES)
        return jnp.concatenate([first, last[:, r * rest : (r + 1) * rest]], axis=-1)

    def phase(p, carry):
        rx_ref[p, 0] = x_ref[p, me]
        whole(x_ref, rx_ref, f_send, f_recv, p).wait_recv()
        for r in range(2):
            normed = cell_norm(base_of(p, r), gain_one_ref[...]).astype(jnp.bfloat16)
            for ref, i in ((k_ref, 1), (v_ref, 2)):
                made = jnp.dot(normed, w_ref[i], preferred_element_type=jnp.float32)
                ref[p, r, :half] = made.astype(jnp.bfloat16)
            made = jnp.dot(normed, w_ref[0], preferred_element_type=jnp.float32)
            q_ref[r] = made.astype(jnp.bfloat16)
        for which in range(2):
            swap(p, which).start()
        for which in range(2):
            swap(p, which).wait_recv()

        lane_head = lax.broadcasted_iota(jnp.int32, (half, width), 1) // head_dim
        results = []
        for r in range(2):

            def one_head(h, carry):
                mine = lane_head == h
                query = jnp.where(mine, q_ref[r].astype(jnp.float32), 0.0).astype(jnp.bfloat16)
                scores = lax.dot_general(
                    query, k_ref[p, r], (((1,), (1,)), ((), ())), preferred_element_type=jnp.float32
                )
                top = jnp.max(scores, axis=-1, keepdims=True)
                expo = jnp.exp2((scores - top) * (head_dim**-0.5 * math.log2(math.e)))
                probs = expo * (1.0 / jnp.sum(expo, axis=-1, keepdims=True))
                got = jnp.dot(
                    probs.astype(jnp.bfloat16), v_ref[p, r], preferred_element_type=jnp.float32
                )
                ctx_ref[...] = jnp.where(mine, got.astype(jnp.bfloat16), ctx_ref[...])
                return carry

            lax.fori_loop(0, HEADS, one_head, 0)
            mid = base_of(p, r) + jnp.dot(
                ctx_ref[...], w_out_ref[...], preferred_element_type=jnp.float32
            )
            normed = cell_norm(mid, gain_two_ref[...]).astype(jnp.bfloat16)
            act = gelu(jnp.dot(normed, w_up_ref[...], preferred_element_type=jnp.float32))
            result = mid + lax.dot_general(
                act.astype(jnp.bfloat16),
                w_down_ref[...],
                (((1,), (1,)), ((), ())),
                preferred_element_type=jnp.float32,
            )
            tx_ref[p, :, r * feats : (r + 1) * feats, :] = (
                result[:, :LANES].astype(jnp.bfloat16).reshape(n, feats, LANES)
            )
            results.append(result[:, LANES:])
        tail = jnp.concatenate(results, axis=-1).astype(jnp.bfloat16)
        tx_ref[p, :, 2 * feats :, :] = tail.reshape(n, feats, LANES)

        send_to(0, n, p)
        own(p).start()
        return carry

    lax.fori_loop(0, phases, phase, 0)

    def drain(p, carry):
        whole(tx_ref, y_ref, b_send, b_recv, p).wait_recv()
        own(p).wait()
        whole(x_ref, rx_ref, f_send, f_recv, p).wait_send()
        whole(tx_ref, y_ref, b_send, b_recv, p).wait_send()
        for which in range(2):
            swap(p, which).wait_send()
        return carry

    lax.fori_loop(0, phases, drain, 0)


def unpack(y_ref, out_ref):
    phases = out_ref.shape[1]
    feats, width = out_ref.shape[3:]
    rest = width - LANES
    for p in range(phases):
        last = y_ref[p, :, 2 * feats :, :].astype(jnp.float32)
        for r in range(2):
            first = y_ref[p, :, r * feats : (r + 1) * feats, :].astype(jnp.float32)
            out_ref[:, p, r, :, :LANES] = first
            out_ref[:, p, r, :, LANES:] = last[:, :, r * rest : (r + 1) * rest]


def solution(mesh):
    groups = mesh.shape["groups"]
    n = mesh.shape["feat"] // CORES
    split = Mesh(mesh.devices.reshape(groups, n, CORES), ("groups", *FEAT))

    def body(
        cells, missing, feat_ids, table, nan_embed, gain_one, w_qkv, w_out, gain_two, w_up, w_down
    ):
        rows, feats, width = cells.shape
        phases = rows // n // 2
        packed = pltpu.VMEM((phases, n, 3 * feats, LANES), jnp.bfloat16)
        half = n * feats
        keys = pltpu.VMEM((phases, 2, CORES * half, width), jnp.bfloat16)
        dma = pltpu.SemaphoreType.DMA
        vmem = pltpu.VMEM
        anywhere = pl.BlockSpec(memory_space=pl.ANY)
        y = pl.pallas_call(
            functools.partial(kernel, n, phases),
            out_shape=jax.ShapeDtypeStruct(packed.shape, jnp.bfloat16),
            in_specs=[anywhere] * 11,
            out_specs=anywhere,
            scratch_shapes=[
                vmem((phases, n, 2, feats, width), cells.dtype),
                vmem((feats, rows), missing.dtype),
                vmem((1, feats), feat_ids.dtype),
                vmem(table.shape, table.dtype),
                vmem((1, width), nan_embed.dtype),
                vmem((1, width), gain_one.dtype),
                vmem(w_qkv.shape, w_qkv.dtype),
                vmem(w_out.shape, w_out.dtype),
                vmem((1, width), gain_two.dtype),
                vmem(w_up.shape, w_up.dtype),
                vmem(w_down.shape[::-1], w_down.dtype),
                packed,
                packed,
                packed,
                vmem((3, width, width), jnp.bfloat16),
                vmem((2, half, width), jnp.bfloat16),
                keys,
                keys,
                vmem((half, width), jnp.bfloat16),
                dma((phases,)),
                dma((10,)),
                dma((phases,)),
                pltpu.SemaphoreType.REGULAR,
                dma((phases,)),
                dma((phases,)),
                dma((phases, 2)),
                dma((phases, 2)),
                dma((phases,)),
                dma((phases,)),
            ],
            compiler_params=pltpu.CompilerParams(collective_id=0, has_side_effects=True),
        )(
            cells.reshape(n, phases, 2, feats, width),
            missing.T,
            feat_ids[None],
            table,
            nan_embed[None],
            gain_one[None],
            w_qkv,
            w_out,
            gain_two[None],
            w_up,
            w_down.T,
        )
        steps = 4 if n % 4 == 0 else 1
        out = pl.pallas_call(
            unpack,
            grid=(steps,),
            out_shape=jax.ShapeDtypeStruct((n, phases, 2, feats, width), jnp.float32),
            in_specs=[pl.BlockSpec((phases, n // steps, 3 * feats, LANES), lambda i: (0, i, 0, 0))],
            out_specs=pl.BlockSpec((n // steps, phases, 2, feats, width), lambda i: (i, 0, 0, 0, 0)),
        )(y)
        return out.reshape(rows, feats, width)

    spread = P("groups", FEAT, None)
    in_specs = (spread, P("groups", FEAT), P(("groups", *FEAT))) + (P(),) * 8
    return jax.shard_map(
        body, mesh=split, in_specs=in_specs, out_specs=spread, check_vma=False
    )
```

```python
import functools
import math

import jax
import jax.numpy as jnp
from jax import lax
from jax.experimental import pallas as pl
from jax.experimental.pallas import tpu as pltpu
from jax.sharding import Mesh
from jax.sharding import PartitionSpec as P

HEADS = 6
CORES = 2
LANES = 128
FEAT = ("chip", "core")
MESH = pl.DeviceIdType.MESH


def cell_norm(values, gain):
    mean = jnp.mean(values, axis=-1, keepdims=True)
    centered = values - mean
    var = jnp.mean(centered * centered, axis=-1, keepdims=True)
    return centered * lax.rsqrt(var + 1e-05) * gain


def gelu(x):
    return 0.5 * x * (1.0 + lax.erf(x * math.sqrt(0.5)))


def kernel(
    n,
    phases,
    cells_hbm,
    missing_hbm,
    ids_hbm,
    table_hbm,
    nan_hbm,
    gain_one_hbm,
    w_qkv_hbm,
    w_out_hbm,
    gain_two_hbm,
    w_up_hbm,
    w_down_hbm,
    y_ref,
    cells_ref,
    missing_ref,
    ids_ref,
    table_ref,
    nan_ref,
    gain_one_ref,
    w_qkv_ref,
    w_out_ref,
    gain_two_ref,
    w_up_ref,
    w_down_ref,
    x_ref,
    rx_ref,
    tx_ref,
    w_ref,
    q_ref,
    k_ref,
    v_ref,
    ctx_ref,
    c_sem,
    in_sem,
    own_sem,
    heard,
    f_send,
    f_recv,
    kv_send,
    kv_recv,
    b_send,
    b_recv,
):
    me = lax.axis_index("chip")
    core = lax.axis_index("core")
    feats, width = cells_ref.shape[3:]
    per_chip = 2 * phases
    rows = n * per_chip
    half = n * feats
    rest = width - LANES
    head_dim = width // HEADS

    def chip_at(k):
        return lax.rem(me + k, n)

    near = n // 4
    barrier = pltpu.get_barrier_semaphore()
    pl.semaphore_signal(barrier, inc=1, device_id={"core": 1 - core}, device_id_type=MESH)
    for k in range(1, n):
        ear = 0 if min(k, n - k) <= near else 1
        pl.semaphore_signal(
            barrier, inc=1, device_id={"chip": chip_at(k), "core": ear}, device_id_type=MESH
        )

    def meet(which, count):
        @pl.when(core == which)
        def _():
            pl.semaphore_wait(barrier, CORES * count + 1)
            pl.semaphore_signal(heard, inc=1, device_id={"core": 1 - core}, device_id_type=MESH)

    def hear(which):
        @pl.when(core != which)
        def _():
            pl.semaphore_wait(heard, 1)

    first = [
        (missing_hbm, missing_ref),
        (ids_hbm, ids_ref),
        (table_hbm, table_ref),
        (nan_hbm, nan_ref),
    ]
    later = [
        (gain_one_hbm, gain_one_ref),
        (w_qkv_hbm, w_qkv_ref),
        (w_out_hbm, w_out_ref),
        (gain_two_hbm, gain_two_ref),
        (w_up_hbm, w_up_ref),
        (w_down_hbm, w_down_ref),
    ]
    loads = [
        pltpu.make_async_copy(src, dst, in_sem.at[i]) for i, (src, dst) in enumerate(first + later)
    ]
    cell_loads = [
        pltpu.make_async_copy(cells_hbm.at[:, p], cells_ref.at[p], c_sem.at[p])
        for p in range(phases)
    ]
    for load in loads[: len(first)] + cell_loads + loads[len(first) :]:
        load.start()
    for load in loads[: len(first)]:
        load.wait()

    spot = lax.broadcasted_iota(jnp.int32, (table_ref.shape[0], feats), 0)
    onehot = (spot == ids_ref[...]).astype(jnp.float32)
    femb = lax.dot_general(
        onehot,
        table_ref[...],
        (((0,), (0,)), ((), ())),
        precision=lax.Precision.HIGHEST,
        preferred_element_type=jnp.float32,
    )
    miss = missing_ref[...].astype(jnp.float32).astype(jnp.bfloat16)
    count = n * 2 * feats

    def make_tokens(p):
        line = lax.broadcasted_iota(jnp.int32, (count, rows), 0) // feats
        column = lax.broadcasted_iota(jnp.int32, (count, rows), 1)
        row = (line // 2) * per_chip + 2 * p + line % 2
        pick = jnp.where(row == column, 1.0, 0.0).astype(jnp.bfloat16)
        spread = lax.dot_general(
            pick, miss, (((1,), (1,)), ((), ())), preferred_element_type=jnp.float32
        )
        line = lax.broadcasted_iota(jnp.int32, (count, feats), 0)
        column = lax.broadcasted_iota(jnp.int32, (count, feats), 1)
        flag = jnp.sum(jnp.where(line % feats == column, spread, 0.0), axis=-1, keepdims=True)
        cell_loads[p].wait()
        tokens = (
            cells_ref[p].astype(jnp.float32)
            + (flag * nan_ref[...]).reshape(n, 2, feats, width)
            + femb[None, None]
        )
        for r in range(2):
            x_ref[p, :, r * feats : (r + 1) * feats, :] = tokens[:, r, :, :LANES].astype(jnp.bfloat16)
        tail = jnp.concatenate([tokens[:, 0, :, LANES:], tokens[:, 1, :, LANES:]], axis=-1)
        x_ref[p, :, 2 * feats :, :] = tail.astype(jnp.bfloat16)

    def forward(p, k):
        return pltpu.make_async_remote_copy(
            src_ref=x_ref.at[p, chip_at(k)],
            dst_ref=rx_ref.at[p, k],
            send_sem=f_send.at[p],
            recv_sem=f_recv.at[p],
            device_id={"chip": chip_at(k)},
            device_id_type=MESH,
        )

    def backward(p, k):
        return pltpu.make_async_remote_copy(
            src_ref=tx_ref.at[p, k],
            dst_ref=y_ref.at[p, me],
            send_sem=b_send.at[p],
            recv_sem=b_recv.at[p],
            device_id={"chip": chip_at(n - k)},
            device_id_type=MESH,
        )

    def send_pairs(copy, p, low, high):
        def pair(i, carry):
            copy(p, high - i).start()
            copy(p, n - high + i).start()
            return carry

        lax.fori_loop(0, high - low + 1, pair, 0)

    def send_to(low, high, *which):
        def one(t, carry):
            @pl.when(t != me)
            def _():
                for p in which:
                    backward(p, lax.rem(me + n - t, n)).start()

            return carry

        lax.fori_loop(low, high, one, 0)

    def whole(src, dst, send, recv, p):
        return pltpu.make_async_remote_copy(
            src_ref=src.at[p, pl.ds(1, n - 1)],
            dst_ref=dst.at[p, pl.ds(1, n - 1)],
            send_sem=send.at[p],
            recv_sem=recv.at[p],
            device_id={"chip": chip_at(1)},
            device_id_type=MESH,
        )

    def swap(p, which):
        ref = (k_ref, v_ref)[which]
        return pltpu.make_async_remote_copy(
            src_ref=ref.at[p, :, pl.ds(0, half)],
            dst_ref=ref.at[p, :, pl.ds(half, half)],
            send_sem=kv_send.at[p, which],
            recv_sem=kv_recv.at[p, which],
            device_id={"core": 1 - core},
            device_id_type=MESH,
        )

    make_tokens(0)
    meet(0, 2 * near)
    hear(0)
    for p in range(phases):
        if p > 0:
            make_tokens(p)
        send_pairs(forward, p, 1, near)
    meet(1, n - 1 - 2 * near)
    hear(1)
    for p in range(phases):
        forward(p, n // 2).start()
        send_pairs(forward, p, near + 1, n // 2 - 1)

    for load in loads[len(first) :]:
        load.wait()
    for i in range(3):
        w_ref[i] = w_qkv_ref[:, i * width : (i + 1) * width]

    def own(p):
        return pltpu.make_async_copy(tx_ref.at[p, 0], y_ref.at[p, me], own_sem.at[p])

    def base_of(p, r):
        first = rx_ref[p, :, r * feats : (r + 1) * feats, :].astype(jnp.float32).reshape(half, LANES)
        last = rx_ref[p, :, 2 * feats :, :].astype(jnp.float32).reshape(half, LANES)
        return jnp.concatenate([first, last[:, r * rest : (r + 1) * rest]], axis=-1)

    def phase(p, carry):
        rx_ref[p, 0] = x_ref[p, me]
        whole(x_ref, rx_ref, f_send, f_recv, p).wait_recv()
        for r in range(2):
            normed = cell_norm(base_of(p, r), gain_one_ref[...]).astype(jnp.bfloat16)
            for ref, i in ((k_ref, 1), (v_ref, 2)):
                made = jnp.dot(normed, w_ref[i], preferred_element_type=jnp.float32)
                ref[p, r, :half] = made.astype(jnp.bfloat16)
            made = jnp.dot(normed, w_ref[0], preferred_element_type=jnp.float32)
            q_ref[r] = made.astype(jnp.bfloat16)
        for which in range(2):
            swap(p, which).start()
        for which in range(2):
            swap(p, which).wait_recv()

        lane_head = lax.broadcasted_iota(jnp.int32, (half, width), 1) // head_dim
        results = []

        def one_head(h, carry):
            mine = lane_head == h
            for r in range(2):
                query = jnp.where(mine, q_ref[r], jnp.zeros_like(q_ref[r]))
                scores = lax.dot_general(
                    query, k_ref[p, r], (((1,), (1,)), ((), ())), preferred_element_type=jnp.float32
                )
                top = jnp.max(scores, axis=-1, keepdims=True)
                expo = jnp.exp2((scores - top) * (head_dim**-0.5 * math.log2(math.e)))
                probs = expo * (1.0 / jnp.sum(expo, axis=-1, keepdims=True))
                got = jnp.dot(
                    probs.astype(jnp.bfloat16), v_ref[p, r], preferred_element_type=jnp.float32
                )
                ctx_ref[r] = jnp.where(mine, got, ctx_ref[r])
            return carry

        lax.fori_loop(0, HEADS, one_head, 0)
        for r in range(2):
            mid = base_of(p, r) + jnp.dot(
                ctx_ref[r].astype(jnp.bfloat16), w_out_ref[...], preferred_element_type=jnp.float32
            )
            normed = cell_norm(mid, gain_two_ref[...]).astype(jnp.bfloat16)
            act = gelu(jnp.dot(normed, w_up_ref[...], preferred_element_type=jnp.float32))
            result = mid + lax.dot_general(
                act.astype(jnp.bfloat16),
                w_down_ref[...],
                (((1,), (1,)), ((), ())),
                preferred_element_type=jnp.float32,
            )
            tx_ref[p, :, r * feats : (r + 1) * feats, :] = (
                result[:, :LANES].astype(jnp.bfloat16).reshape(n, feats, LANES)
            )
            results.append(result[:, LANES:])
        tail = jnp.concatenate(results, axis=-1).astype(jnp.bfloat16)
        tx_ref[p, :, 2 * feats :, :] = tail.reshape(n, feats, LANES)


        @pl.when(p == 0)
        def _():
            send_to(0, n, p)

        own(p).start()
        return carry

    lax.fori_loop(0, phases, phase, 0)
    send_to(0, n, 1, 2)

    def drain(p, carry):
        whole(tx_ref, y_ref, b_send, b_recv, p).wait_recv()
        own(p).wait()
        whole(x_ref, rx_ref, f_send, f_recv, p).wait_send()
        whole(tx_ref, y_ref, b_send, b_recv, p).wait_send()
        for which in range(2):
            swap(p, which).wait_send()
        return carry

    lax.fori_loop(0, phases, drain, 0)


def unpack(y_ref, out_ref):
    phases = out_ref.shape[1]
    feats, width = out_ref.shape[3:]
    rest = width - LANES
    for p in range(phases):
        last = y_ref[p, :, 2 * feats :, :].astype(jnp.float32)
        for r in range(2):
            first = y_ref[p, :, r * feats : (r + 1) * feats, :].astype(jnp.float32)
            out_ref[:, p, r, :, :LANES] = first
            out_ref[:, p, r, :, LANES:] = last[:, :, r * rest : (r + 1) * rest]


def solution(mesh):
    groups = mesh.shape["groups"]
    n = mesh.shape["feat"] // CORES
    split = Mesh(mesh.devices.reshape(groups, n, CORES), ("groups", *FEAT))

    def body(
        cells, missing, feat_ids, table, nan_embed, gain_one, w_qkv, w_out, gain_two, w_up, w_down
    ):
        rows, feats, width = cells.shape
        phases = rows // n // 2
        packed = pltpu.VMEM((phases, n, 3 * feats, LANES), jnp.bfloat16)
        half = n * feats
        keys = pltpu.VMEM((phases, 2, CORES * half, width), jnp.bfloat16)
        dma = pltpu.SemaphoreType.DMA
        vmem = pltpu.VMEM
        anywhere = pl.BlockSpec(memory_space=pl.ANY)
        y = pl.pallas_call(
            functools.partial(kernel, n, phases),
            out_shape=jax.ShapeDtypeStruct(packed.shape, jnp.bfloat16),
            in_specs=[anywhere] * 11,
            out_specs=anywhere,
            scratch_shapes=[
                vmem((phases, n, 2, feats, width), cells.dtype),
                vmem((feats, rows), missing.dtype),
                vmem((1, feats), feat_ids.dtype),
                vmem(table.shape, table.dtype),
                vmem((1, width), nan_embed.dtype),
                vmem((1, width), gain_one.dtype),
                vmem(w_qkv.shape, w_qkv.dtype),
                vmem(w_out.shape, w_out.dtype),
                vmem((1, width), gain_two.dtype),
                vmem(w_up.shape, w_up.dtype),
                vmem(w_down.shape[::-1], w_down.dtype),
                packed,
                packed,
                packed,
                vmem((3, width, width), jnp.bfloat16),
                vmem((2, half, width), jnp.bfloat16),
                keys,
                keys,
                vmem((2, half, width), jnp.float32),
                dma((phases,)),
                dma((10,)),
                dma((phases,)),
                pltpu.SemaphoreType.REGULAR,
                dma((phases,)),
                dma((phases,)),
                dma((phases, 2)),
                dma((phases, 2)),
                dma((phases,)),
                dma((phases,)),
            ],
            compiler_params=pltpu.CompilerParams(collective_id=0, has_side_effects=True),
        )(
            cells.reshape(n, phases, 2, feats, width),
            missing.T,
            feat_ids[None],
            table,
            nan_embed[None],
            gain_one[None],
            w_qkv,
            w_out,
            gain_two[None],
            w_up,
            w_down.T,
        )
        steps = 2
        out = pl.pallas_call(
            unpack,
            grid=(steps,),
            out_shape=jax.ShapeDtypeStruct((n, phases, 2, feats, width), jnp.float32),
            in_specs=[pl.BlockSpec((phases, n // steps, 3 * feats, LANES), lambda i: (0, i, 0, 0))],
            out_specs=pl.BlockSpec((n // steps, phases, 2, feats, width), lambda i: (i, 0, 0, 0, 0)),
        )(y)
        return out.reshape(rows, feats, width)

    spread = P("groups", FEAT, None)
    in_specs = (spread, P("groups", FEAT), P(("groups", *FEAT))) + (P(),) * 8
    return jax.shard_map(
        body, mesh=split, in_specs=in_specs, out_specs=spread, check_vma=False
    )
```

```python
import functools
import math

import jax
import jax.numpy as jnp
from jax import lax
from jax.experimental import pallas as pl
from jax.experimental.pallas import tpu as pltpu
from jax.sharding import Mesh
from jax.sharding import PartitionSpec as P

HEADS = 6
CORES = 2
LANES = 128
FEAT = ("chip", "core")
MESH = pl.DeviceIdType.MESH


def cell_norm(values, gain):
    mean = jnp.mean(values, axis=-1, keepdims=True)
    centered = values - mean
    var = jnp.mean(centered * centered, axis=-1, keepdims=True)
    return centered * lax.rsqrt(var + 1e-05) * gain


def gelu(x):
    return 0.5 * x * (1.0 + lax.erf(x * math.sqrt(0.5)))


def kernel(
    n,
    phases,
    cells_hbm,
    missing_hbm,
    ids_hbm,
    table_hbm,
    nan_hbm,
    gain_one_hbm,
    w_qkv_hbm,
    w_out_hbm,
    gain_two_hbm,
    w_up_hbm,
    w_down_hbm,
    y_ref,
    cells_ref,
    missing_ref,
    ids_ref,
    table_ref,
    nan_ref,
    gain_one_ref,
    w_qkv_ref,
    w_out_ref,
    gain_two_ref,
    w_up_ref,
    w_down_ref,
    x_ref,
    rx_ref,
    tx_ref,
    w_ref,
    q_ref,
    k_ref,
    v_ref,
    ctx_ref,
    c_sem,
    in_sem,
    own_sem,
    heard,
    f_send,
    f_recv,
    kv_send,
    kv_recv,
    b_send,
    b_recv,
):
    me = lax.axis_index("chip")
    core = lax.axis_index("core")
    feats, width = cells_ref.shape[3:]
    per_chip = 2 * phases
    rows = n * per_chip
    half = n * feats
    rest = width - LANES
    head_dim = width // HEADS

    def chip_at(k):
        return lax.rem(me + k, n)

    near = n // 4
    barrier = pltpu.get_barrier_semaphore()
    pl.semaphore_signal(barrier, inc=1, device_id={"core": 1 - core}, device_id_type=MESH)
    for k in range(1, n):
        ear = 0 if min(k, n - k) <= near else 1
        pl.semaphore_signal(
            barrier, inc=1, device_id={"chip": chip_at(k), "core": ear}, device_id_type=MESH
        )

    def meet(which, count):
        @pl.when(core == which)
        def _():
            pl.semaphore_wait(barrier, CORES * count + 1)
            pl.semaphore_signal(heard, inc=1, device_id={"core": 1 - core}, device_id_type=MESH)

    def hear(which):
        @pl.when(core != which)
        def _():
            pl.semaphore_wait(heard, 1)

    first = [
        (missing_hbm, missing_ref),
        (ids_hbm, ids_ref),
        (table_hbm, table_ref),
        (nan_hbm, nan_ref),
    ]
    later = [
        (gain_one_hbm, gain_one_ref),
        (w_qkv_hbm, w_qkv_ref),
        (w_out_hbm, w_out_ref),
        (gain_two_hbm, gain_two_ref),
        (w_up_hbm, w_up_ref),
        (w_down_hbm, w_down_ref),
    ]
    loads = [
        pltpu.make_async_copy(src, dst, in_sem.at[i]) for i, (src, dst) in enumerate(first + later)
    ]
    cell_loads = [
        pltpu.make_async_copy(cells_hbm.at[:, p], cells_ref.at[p], c_sem.at[p])
        for p in range(phases)
    ]
    for load in loads[: len(first)] + cell_loads + loads[len(first) :]:
        load.start()
    for load in loads[: len(first)]:
        load.wait()

    spot = lax.broadcasted_iota(jnp.int32, (table_ref.shape[0], feats), 0)
    onehot = (spot == ids_ref[...]).astype(jnp.float32)
    femb = lax.dot_general(
        onehot,
        table_ref[...],
        (((0,), (0,)), ((), ())),
        precision=lax.Precision.HIGHEST,
        preferred_element_type=jnp.float32,
    )
    miss = missing_ref[...].astype(jnp.float32).astype(jnp.bfloat16)
    count = n * 2 * feats

    def make_tokens(p):
        line = lax.broadcasted_iota(jnp.int32, (count, rows), 0) // feats
        column = lax.broadcasted_iota(jnp.int32, (count, rows), 1)
        row = (line // 2) * per_chip + 2 * p + line % 2
        pick = jnp.where(row == column, 1.0, 0.0).astype(jnp.bfloat16)
        spread = lax.dot_general(
            pick, miss, (((1,), (1,)), ((), ())), preferred_element_type=jnp.float32
        )
        line = lax.broadcasted_iota(jnp.int32, (count, feats), 0)
        column = lax.broadcasted_iota(jnp.int32, (count, feats), 1)
        flag = jnp.sum(jnp.where(line % feats == column, spread, 0.0), axis=-1, keepdims=True)
        cell_loads[p].wait()
        tokens = (
            cells_ref[p].astype(jnp.float32)
            + (flag * nan_ref[...]).reshape(n, 2, feats, width)
            + femb[None, None]
        )
        for r in range(2):
            x_ref[p, :, r * feats : (r + 1) * feats, :] = tokens[:, r, :, :LANES].astype(jnp.bfloat16)
        tail = jnp.concatenate([tokens[:, 0, :, LANES:], tokens[:, 1, :, LANES:]], axis=-1)
        x_ref[p, :, 2 * feats :, :] = tail.astype(jnp.bfloat16)

    def forward(p, k):
        return pltpu.make_async_remote_copy(
            src_ref=x_ref.at[p, chip_at(k)],
            dst_ref=rx_ref.at[p, k],
            send_sem=f_send.at[p],
            recv_sem=f_recv.at[p],
            device_id={"chip": chip_at(k)},
            device_id_type=MESH,
        )

    def backward(p, k):
        return pltpu.make_async_remote_copy(
            src_ref=tx_ref.at[p, k],
            dst_ref=y_ref.at[p, me],
            send_sem=b_send.at[p],
            recv_sem=b_recv.at[p],
            device_id={"chip": chip_at(n - k)},
            device_id_type=MESH,
        )

    def send_pairs(copy, p, low, high):
        def pair(i, carry):
            copy(p, high - i).start()
            copy(p, n - high + i).start()
            return carry

        lax.fori_loop(0, high - low + 1, pair, 0)

    def send_to(low, high, *which):
        def one(t, carry):
            @pl.when(t != me)
            def _():
                for p in which:
                    backward(p, lax.rem(me + n - t, n)).start()

            return carry

        lax.fori_loop(low, high, one, 0)

    def whole(src, dst, send, recv, p):
        return pltpu.make_async_remote_copy(
            src_ref=src.at[p, pl.ds(1, n - 1)],
            dst_ref=dst.at[p, pl.ds(1, n - 1)],
            send_sem=send.at[p],
            recv_sem=recv.at[p],
            device_id={"chip": chip_at(1)},
            device_id_type=MESH,
        )

    def swap(p, which):
        ref = (k_ref, v_ref)[which]
        return pltpu.make_async_remote_copy(
            src_ref=ref.at[p, :, pl.ds(0, half)],
            dst_ref=ref.at[p, :, pl.ds(half, half)],
            send_sem=kv_send.at[p, which],
            recv_sem=kv_recv.at[p, which],
            device_id={"core": 1 - core},
            device_id_type=MESH,
        )

    make_tokens(0)
    meet(0, 2 * near)
    hear(0)
    for p in range(phases):
        if p > 0:
            make_tokens(p)
        send_pairs(forward, p, 1, near)
    meet(1, n - 1 - 2 * near)
    hear(1)
    for p in range(phases):
        forward(p, n // 2).start()
        send_pairs(forward, p, near + 1, n // 2 - 1)

    for load in loads[len(first) :]:
        load.wait()
    for i in range(3):
        w_ref[i] = w_qkv_ref[:, i * width : (i + 1) * width]

    def own(p):
        return pltpu.make_async_copy(tx_ref.at[p, 0], y_ref.at[p, me], own_sem.at[p])

    def base_of(p, r):
        first = rx_ref[p, :, r * feats : (r + 1) * feats, :].astype(jnp.float32).reshape(half, LANES)
        last = rx_ref[p, :, 2 * feats :, :].astype(jnp.float32).reshape(half, LANES)
        return jnp.concatenate([first, last[:, r * rest : (r + 1) * rest]], axis=-1)

    def phase(p, carry):
        rx_ref[p, 0] = x_ref[p, me]
        whole(x_ref, rx_ref, f_send, f_recv, p).wait_recv()
        for r in range(2):
            normed = cell_norm(base_of(p, r), gain_one_ref[...]).astype(jnp.bfloat16)
            for ref, i in ((k_ref, 1), (v_ref, 2)):
                made = jnp.dot(normed, w_ref[i], preferred_element_type=jnp.float32)
                ref[p, r, :half] = made.astype(jnp.bfloat16)
            made = jnp.dot(normed, w_ref[0], preferred_element_type=jnp.float32)
            q_ref[r] = made.astype(jnp.bfloat16)
        for which in range(2):
            swap(p, which).start()
        for which in range(2):
            swap(p, which).wait_recv()

        lane_head = lax.broadcasted_iota(jnp.int32, (half, width), 1) // head_dim
        results = []

        def one_head(h, carry):
            mine = lane_head == h
            for r in range(2):
                query = jnp.where(mine, q_ref[r], jnp.zeros_like(q_ref[r]))
                scores = lax.dot_general(
                    query, k_ref[p, r], (((1,), (1,)), ((), ())), preferred_element_type=jnp.float32
                )
                top = jnp.max(scores, axis=-1, keepdims=True)
                expo = jnp.exp2((scores - top) * (head_dim**-0.5 * math.log2(math.e)))
                probs = expo * (1.0 / jnp.sum(expo, axis=-1, keepdims=True))
                got = jnp.dot(
                    probs.astype(jnp.bfloat16), v_ref[p, r], preferred_element_type=jnp.float32
                )
                ctx_ref[r] = jnp.where(mine, got, ctx_ref[r])
            return carry

        lax.fori_loop(0, HEADS, one_head, 0, unroll=2)
        for r in range(2):
            mid = base_of(p, r) + jnp.dot(
                ctx_ref[r].astype(jnp.bfloat16), w_out_ref[...], preferred_element_type=jnp.float32
            )
            normed = cell_norm(mid, gain_two_ref[...]).astype(jnp.bfloat16)
            act = gelu(jnp.dot(normed, w_up_ref[...], preferred_element_type=jnp.float32))
            result = mid + lax.dot_general(
                act.astype(jnp.bfloat16),
                w_down_ref[...],
                (((1,), (1,)), ((), ())),
                preferred_element_type=jnp.float32,
            )
            tx_ref[p, :, r * feats : (r + 1) * feats, :] = (
                result[:, :LANES].astype(jnp.bfloat16).reshape(n, feats, LANES)
            )
            results.append(result[:, LANES:])
        tail = jnp.concatenate(results, axis=-1).astype(jnp.bfloat16)
        tx_ref[p, :, 2 * feats :, :] = tail.reshape(n, feats, LANES)


        @pl.when(p == 0)
        def _():
            send_to(0, n, p)

        own(p).start()
        return carry

    lax.fori_loop(0, phases, phase, 0)
    send_to(0, n, 1, 2)

    def drain(p, carry):
        whole(tx_ref, y_ref, b_send, b_recv, p).wait_recv()
        own(p).wait()
        whole(x_ref, rx_ref, f_send, f_recv, p).wait_send()
        whole(tx_ref, y_ref, b_send, b_recv, p).wait_send()
        for which in range(2):
            swap(p, which).wait_send()
        return carry

    lax.fori_loop(0, phases, drain, 0)


def unpack(y_ref, out_ref):
    phases = out_ref.shape[1]
    feats, width = out_ref.shape[3:]
    rest = width - LANES
    for p in range(phases):
        last = y_ref[p, :, 2 * feats :, :].astype(jnp.float32)
        for r in range(2):
            first = y_ref[p, :, r * feats : (r + 1) * feats, :].astype(jnp.float32)
            out_ref[:, p, r, :, :LANES] = first
            out_ref[:, p, r, :, LANES:] = last[:, :, r * rest : (r + 1) * rest]


def solution(mesh):
    groups = mesh.shape["groups"]
    n = mesh.shape["feat"] // CORES
    split = Mesh(mesh.devices.reshape(groups, n, CORES), ("groups", *FEAT))

    def body(
        cells, missing, feat_ids, table, nan_embed, gain_one, w_qkv, w_out, gain_two, w_up, w_down
    ):
        rows, feats, width = cells.shape
        phases = rows // n // 2
        packed = pltpu.VMEM((phases, n, 3 * feats, LANES), jnp.bfloat16)
        half = n * feats
        keys = pltpu.VMEM((phases, 2, CORES * half, width), jnp.bfloat16)
        dma = pltpu.SemaphoreType.DMA
        vmem = pltpu.VMEM
        anywhere = pl.BlockSpec(memory_space=pl.ANY)
        y = pl.pallas_call(
            functools.partial(kernel, n, phases),
            out_shape=jax.ShapeDtypeStruct(packed.shape, jnp.bfloat16),
            in_specs=[anywhere] * 11,
            out_specs=anywhere,
            scratch_shapes=[
                vmem((phases, n, 2, feats, width), cells.dtype),
                vmem((feats, rows), missing.dtype),
                vmem((1, feats), feat_ids.dtype),
                vmem(table.shape, table.dtype),
                vmem((1, width), nan_embed.dtype),
                vmem((1, width), gain_one.dtype),
                vmem(w_qkv.shape, w_qkv.dtype),
                vmem(w_out.shape, w_out.dtype),
                vmem((1, width), gain_two.dtype),
                vmem(w_up.shape, w_up.dtype),
                vmem(w_down.shape[::-1], w_down.dtype),
                packed,
                packed,
                packed,
                vmem((3, width, width), jnp.bfloat16),
                vmem((2, half, width), jnp.bfloat16),
                keys,
                keys,
                vmem((2, half, width), jnp.float32),
                dma((phases,)),
                dma((10,)),
                dma((phases,)),
                pltpu.SemaphoreType.REGULAR,
                dma((phases,)),
                dma((phases,)),
                dma((phases, 2)),
                dma((phases, 2)),
                dma((phases,)),
                dma((phases,)),
            ],
            compiler_params=pltpu.CompilerParams(collective_id=0, has_side_effects=True),
        )(
            cells.reshape(n, phases, 2, feats, width),
            missing.T,
            feat_ids[None],
            table,
            nan_embed[None],
            gain_one[None],
            w_qkv,
            w_out,
            gain_two[None],
            w_up,
            w_down.T,
        )
        steps = 2
        out = pl.pallas_call(
            unpack,
            grid=(steps,),
            out_shape=jax.ShapeDtypeStruct((n, phases, 2, feats, width), jnp.float32),
            in_specs=[pl.BlockSpec((phases, n // steps, 3 * feats, LANES), lambda i: (0, i, 0, 0))],
            out_specs=pl.BlockSpec((n // steps, phases, 2, feats, width), lambda i: (i, 0, 0, 0, 0)),
        )(y)
        return out.reshape(rows, feats, width)

    spread = P("groups", FEAT, None)
    in_specs = (spread, P("groups", FEAT), P(("groups", *FEAT))) + (P(),) * 8
    return jax.shard_map(
        body, mesh=split, in_specs=in_specs, out_specs=spread, check_vma=False
    )
```
